32 devices in a mesh: seq: 4 (over y, x), dp: 8 (over z, core).
Axes of the slice: x: 2, y: 2, z: 4, core: 2. Of those that a mesh axis runs over, the one named last changes fastest.
Arguments:
- tokens_in: bfloat16 [8, 1024, 2560], P('dp', 'seq'), may hold values from -6 to 6
- step_raw: bfloat16 [8, 1024, 40], P('dp', 'seq'), may hold values from -3 to 3
- input_map: bfloat16 [8, 1024, 128], P('dp', 'seq'), may hold values from -1.796875 to 1.796875
- output_map: bfloat16 [8, 1024, 128], P('dp', 'seq'), may hold values from -1.796875 to 1.796875
- decay_log: float32 [40], replicated
- skip_gain: float32 [40], replicated, may hold values from 0.5 to 1.5
- step_bias: float32 [40], replicated, may hold values from -4.7 to -2.2
- grad_out: bfloat16 [8, 1024, 2560], P('dp', 'seq'), may hold values from -6 to 6
Outputs:
- grad_tokens: bfloat16 [8, 1024, 2560], P('dp', 'seq')
- grad_steps: float32 [8, 1024, 40], P('dp', 'seq')
- grad_input_map: float32 [8, 1024, 128], P('dp', 'seq')
- grad_output_map: float32 [8, 1024, 128], P('dp', 'seq')
- grad_decay_log: float32 [40], replicated
- grad_skip_gain: float32 [40], replicated
- grad_step_bias: float32 [40], replicated
The draws below stay inside these ranges and needn't reach their ends.
All inputs are finite; a program needn't handle non-finite values.
Results may differ from the reference program's by a relative error of at most 0.001.
Values may be sent and summed in bfloat16 or wider, within the bound.
A program may use at most 192 MiB of HBM per device.

```python
import math
import jax
import jax.numpy as jnp
from jax import lax

HEADS = 40
HEADDIM = 64
STATE = 128
SPAN = 256
HEAD_BLOCK = 8
TOK_DEV = 256
LENGTH = 1024
GROUPS = 8


def head_rates(key):
    slow_pick = jax.random.randint(jax.random.fold_in(key, 101), (HEADS,), 0, 10)
    slow_heads = slow_pick < 5
    slow_rate = jnp.exp(jax.random.uniform(jax.random.fold_in(key, 102), (HEADS,), jnp.float32, math.log(0.1), math.log(1.5))) / LENGTH
    fast_rate = jnp.exp(jax.random.uniform(jax.random.fold_in(key, 103), (HEADS,), jnp.float32, math.log(0.02), math.log(0.1)))
    base_step = jnp.exp(jax.random.uniform(jax.random.fold_in(key, 104), (HEADS,), jnp.float32, math.log(0.01), math.log(0.1)))
    return (jnp.where(slow_heads, slow_rate, fast_rate), base_step)


def draw_decay_log(key, part):
    per_token, base_step = head_rates(key)
    return jnp.log(per_token / base_step)


def draw_step_bias(key, part):
    per_token, base_step = head_rates(key)
    return jnp.log(jnp.expm1(base_step))


def draw_step_raw(key, part):
    noise_key = jax.random.fold_in(key, 201)
    noise = 0.5 * jax.random.truncated_normal(noise_key, -4.0, 4.0, (GROUPS, LENGTH, HEADS), jnp.float32)
    offsets = jax.random.uniform(jax.random.fold_in(key, 202), (GROUPS, LENGTH // TOK_DEV, HEADS), jnp.float32, -0.7, 0.7)
    return (noise + jnp.repeat(offsets, TOK_DEV, axis=1)).astype(jnp.bfloat16)


def block_levels(own_key, dims, pieces, smallest, top_value):
    def one(position, blocks):
        steps = jax.random.uniform(jax.random.fold_in(jax.random.fold_in(own_key, 6), position), (blocks,), jnp.float32, smallest / len(pieces), top_value / len(pieces))
        return jnp.repeat(jnp.exp(steps), dims[position] // blocks).reshape((-1,) + (1,) * (len(dims) - position - 1))

    gain = one(*pieces[0])
    for cut in pieces[1:]:
        gain = gain * one(*cut)
    return gain


def normal_values(key, dims, scale, most, pieces=(), kind=jnp.bfloat16):
    drawn = jax.random.normal(key, dims, jnp.float32) * scale
    if len(pieces) > 0:
        drawn = block_levels(key, dims, pieces, -0.22, 0.18) * drawn
    return jnp.clip(drawn, min=-most, max=most).astype(kind)


def setup_inputs(seed: int = 0) -> dict:
    keys = jax.random.split(jax.random.key(seed), 9)
    return {
        "tokens_in": normal_values(keys[0], (GROUPS, LENGTH, HEADS * HEADDIM), 1.0, 6.0, ((0, 8), (1, 4))),
        "step_raw": draw_step_raw(jax.random.fold_in(keys[8], 71), 0),
        "input_map": normal_values(keys[2], (GROUPS, LENGTH, STATE), 0.3, 1.796875, ((0, 8), (1, 4))),
        "output_map": normal_values(keys[3], (GROUPS, LENGTH, STATE), 0.3, 1.796875, ((0, 8), (1, 4))),
        "decay_log": draw_decay_log(jax.random.fold_in(keys[8], 71), 0),
        "skip_gain": jnp.clip(jax.random.uniform(keys[5], (HEADS,), jnp.float32, 0.5, 1.5), 0.5, 1.5),
        "step_bias": draw_step_bias(jax.random.fold_in(keys[8], 71), 0),
        "grad_out": normal_values(keys[7], (GROUPS, LENGTH, HEADS * HEADDIM), 1.0, 6.0, ((0, 8), (1, 4))),
    }


highest = lax.Precision.HIGHEST

def block_forward(head_block, input_rows, output_rows):
    values, step_sizes, decay_rates, skip_part, state_in = head_block
    length = values.shape[0]
    span_count = length // SPAN
    head_count = decay_rates.shape[0]
    head_width = values.shape[2]
    log_decay = -decay_rates[None, :] * step_sizes
    scaled = values * step_sizes[:, :, None]
    causal = lax.broadcasted_iota(jnp.int32, (SPAN, SPAN), 0) >= lax.broadcasted_iota(jnp.int32, (SPAN, SPAN), 1)

    def advance(state_now, span_item):
        span_in, span_decay, span_b, span_c = span_item
        running = jnp.cumsum(span_decay, axis=0)
        scores = jnp.dot(span_c, span_b.T, precision=highest)
        spread = running.T[:, :, None] - running.T[:, None, :]
        weights = jnp.exp(jnp.where(causal[None], spread, -jnp.inf)) * scores[None]
        inside = jnp.einsum('hts,shp->thp', weights, span_in, precision=highest)
        carried = jnp.einsum('tn,hpn->thp', span_c, state_now, precision=highest) * jnp.exp(running)[:, :, None]
        last_sum = running[-1]
        tail_weight = jnp.exp(last_sum[None, :] - running)
        fresh_state = jnp.einsum('shp,sn->hpn', span_in * tail_weight[:, :, None], span_b, precision=highest)
        return (jnp.exp(last_sum)[:, None, None] * state_now + fresh_state, inside + carried)
    span_items = (scaled.reshape(span_count, SPAN, head_count, head_width), log_decay.reshape(span_count, SPAN, head_count), input_rows.reshape(span_count, SPAN, -1), output_rows.reshape(span_count, SPAN, -1))
    state_out, outputs = lax.scan(advance, state_in, span_items)
    result = outputs.reshape(length, head_count, head_width) + skip_part[None, :, None] * values
    return (result, state_out)

def segment(values, raw_steps, input_rows, output_rows, decay_log, skip_gain, step_bias, state_in):
    length = values.shape[0]
    head_count = decay_log.shape[0]
    head_width = values.shape[1] // head_count
    state_size = input_rows.shape[1]
    per_block = math.gcd(HEAD_BLOCK, head_count)
    blocks = head_count // per_block
    step_sizes = jax.nn.softplus(raw_steps + step_bias[None, :])
    decay_rates = jnp.exp(decay_log)
    packed = (values.reshape(length, blocks, per_block, head_width).transpose(1, 0, 2, 3), step_sizes.reshape(length, blocks, per_block).transpose(1, 0, 2), decay_rates.reshape(blocks, per_block), skip_gain.reshape(blocks, per_block), state_in.reshape(blocks, per_block, head_width, state_size))
    results, finals = lax.map(lambda head_block: block_forward(head_block, input_rows, output_rows), packed)
    return (results.transpose(1, 0, 2, 3).reshape(length, head_count * head_width), finals.reshape(head_count, head_width, state_size))

def reference(tokens_in, step_raw, input_map, output_map, decay_log, skip_gain, step_bias, grad_out):
    zero_state = jnp.zeros((HEADS, HEADDIM, STATE), jnp.float32)

    def one_group(group_item):
        token_rows, raw_rows, input_rows, output_rows, cotangent = [member.astype(jnp.float32) for member in group_item]
        output, pullback = jax.vjp(lambda primals: segment(*primals, zero_state)[0], (token_rows, raw_rows, input_rows, output_rows, decay_log, skip_gain, step_bias))
        return pullback(cotangent)[0]
    gradients = lax.map(one_group, (tokens_in, step_raw, input_map, output_map, grad_out))
    factor = 1.0 / math.sqrt(GROUPS * LENGTH * HEADDIM)
    return (gradients[0].astype(jnp.bfloat16), gradients[1], gradients[2], gradients[3], lax.optimization_barrier(jnp.sum(gradients[4], axis=0)) * factor, lax.optimization_barrier(jnp.sum(gradients[5], axis=0)) * factor, lax.optimization_barrier(jnp.sum(gradients[6], axis=0)) * factor)
```

```python
import functools
import math

import jax
import jax.numpy as jnp
from jax import lax
from jax.experimental import pallas as pl
from jax.experimental.pallas import tpu as pltpu
from jax.sharding import PartitionSpec as P

F32 = jnp.float32
BF16 = jnp.bfloat16
LANES = 128
EXTRA = 8
WIRE = jnp.float32


def dot(a, b, dims=((1,), (0,))):
    return lax.dot_general(a, b, (dims, ((), ())), preferred_element_type=F32)


def split2(v):
    hi = v.astype(BF16)
    return hi, (v - hi.astype(F32)).astype(BF16)


def split3(v):
    hi = v.astype(BF16)
    rest = v - hi.astype(F32)
    mid = rest.astype(BF16)
    return hi, mid, (rest - mid.astype(F32)).astype(BF16)


def exact_sum(mask, v):
    a, b, c = split3(v)
    return dot(mask, a) + (dot(mask, b) + dot(mask, c))


def expand(columns, first, count, width):
    rows = columns.shape[0]
    per = LANES // width
    lane = lax.broadcasted_iota(jnp.int32, (rows, LANES), 1)
    out = []
    for j in range(0, count, per):
        value = jnp.broadcast_to(columns[:, first + j : first + j + 1], (rows, LANES))
        for k in range(1, per):
            more = jnp.broadcast_to(columns[:, first + j + k : first + j + k + 1], (rows, LANES))
            value = jnp.where(lane < k * width, value, more)
        out.append(value)
    return jnp.concatenate(out, axis=1)


def turn(columns, by):
    return pltpu.roll(columns, lax.rem(LANES - by, LANES), 1)


def state_kernel(
    n, per, width, me_ref, raw_ref, bias_ref, rate_ref, b_ref, c_ref, x_ref, g_ref, *refs
):
    sends = refs[: n - 1]
    dt_ref, run_ref, run_t_ref, sig_ref, into_ref, grow_ref, scr, bt_ref, ct_ref = refs[n - 1 :]
    step = pl.program_id(0)
    heads = raw_ref.shape[1]
    length = raw_ref.shape[0]

    @pl.when(step == 0)
    def _():
        scr[...] = jnp.zeros_like(scr)
        scr[:, :heads] = raw_ref[...].astype(F32) + bias_ref[...]
        value = scr[...]
        dt = jnp.maximum(value, 0.0) + jnp.log1p(jnp.exp(-jnp.abs(value)))
        dt_ref[...] = dt
        sig_ref[...] = 1.0 / (1.0 + jnp.exp(-value))
        scr[0:1, :heads] = jnp.exp(rate_ref[...])
        decay = -scr[0:1, :] * dt
        row = lax.broadcasted_iota(jnp.int32, (length, length), 0)
        col = lax.broadcasted_iota(jnp.int32, (length, length), 1)
        lower = jnp.where(row >= col, 1.0, 0.0).astype(BF16)
        running = exact_sum(lower, decay)
        run_ref[...] = running
        run_t_ref[...] = running.T
        into_ref[...] = jnp.exp(running[length - 1 : length] - running) * dt
        grow_ref[...] = jnp.exp(running)
        bt_ref[...] = b_ref[...].astype(F32).T.astype(BF16)
        ct_ref[...] = c_ref[...].astype(F32).T.astype(BF16)

    me = me_ref[0]
    first = step * per
    into = turn(into_ref[...], first)
    grow = turn(grow_ref[...], first)
    last = turn(run_ref[length - EXTRA : length, :], first)
    xw = x_ref[...].astype(F32) * expand(into, 0, per, width)
    gw = g_ref[...].astype(F32) * expand(grow, 0, per, width)
    x_hi, x_lo = split2(xw)
    g_hi, g_lo = split2(gw)
    states = bt_ref.shape[0]
    state = dot(bt_ref[...], x_hi) + dot(bt_ref[...], x_lo)
    grad = dot(ct_ref[...], g_hi) + dot(ct_ref[...], g_lo)
    extra = expand(last, 0, per, width)
    for k in range(1, n):
        sends[k - 1][:states, :] = jnp.where(me + k < n, state, grad).astype(WIRE)
        sends[k - 1][states:, :] = extra.astype(WIRE)


def inside_kernel(
    per, width, run_ref, run_t_ref, dt_ref, b_ref, c_ref, x_ref, g_ref,
    gx_ref, rows_ref, db_ref, dc_ref, cb_ref, acc_ref,
):
    step = pl.program_id(0)
    length = run_ref.shape[0]
    tile = LANES
    nt = ((1,), (1,))

    @pl.when(step == 0)
    def _():
        cb_ref[...] = dot(b_ref[...], c_ref[...], nt)
        acc_ref[...] = jnp.zeros_like(acc_ref)

    run = turn(run_ref[...], step * per)
    dt = turn(dt_ref[...], step * per)
    group = LANES // width
    lane = lax.broadcasted_iota(jnp.int32, (1, LANES), 1)
    causal = lax.broadcasted_iota(jnp.int32, (tile, tile), 0) <= lax.broadcasted_iota(
        jnp.int32, (tile, tile), 1
    )
    for pair in range(per // group):
        x_pair = x_ref[:, pair * LANES : (pair + 1) * LANES]
        g_pair = g_ref[:, pair * LANES : (pair + 1) * LANES]
        zero = jnp.zeros_like(g_pair)
        totals = [None] * (length // tile)
        for k in range(group):
            head = pair * group + k
            own = (lane >= k * width) & (lane < (k + 1) * width)
            g_own = jnp.where(own, g_pair, zero)
            column_sums = [None] * (length // tile)
            for sb in range(length // tile):
                rows = slice(sb * tile, (sb + 1) * tile)
                t0 = sb * tile
                dw = dot(x_pair[rows], g_own[t0:], nt)
                run_s = jnp.broadcast_to(run[rows, head : head + 1], (tile, tile))
                dt_s = jnp.broadcast_to(dt[rows, head : head + 1], (tile, tile))
                parts_hi, parts_lo = [], []
                for tb in range(sb, length // tile):
                    cols = slice(tb * tile, (tb + 1) * tile)
                    spread = run_t_ref[head : head + 1, cols] - run_s
                    if tb == sb:
                        spread = jnp.where(causal, spread, -jnp.inf)
                    q = jnp.exp(spread) * dt_s
                    dw_t = dw[:, tb * tile - t0 : (tb + 1) * tile - t0]
                    w = q * cb_ref[rows, cols]
                    acc_ref[rows, cols] += q * dw_t
                    part = jnp.sum(w * dw_t, axis=0, keepdims=True)
                    column_sums[tb] = part if column_sums[tb] is None else column_sums[tb] + part
                    hi, lo = split2(w)
                    parts_hi.append(hi)
                    parts_lo.append(lo)
                w_hi = jnp.concatenate(parts_hi, axis=1)
                w_lo = jnp.concatenate(parts_lo, axis=1)
                out = dot(w_hi, g_own[t0:]) + dot(w_lo, g_own[t0:])
                totals[sb] = out if totals[sb] is None else totals[sb] + out
            for tb in range(length // tile):
                rows_ref[head : head + 1, tb * tile : (tb + 1) * tile] = column_sums[tb]
        for sb in range(length // tile):
            gx_ref[sb * tile : (sb + 1) * tile, pair * LANES : (pair + 1) * LANES] = totals[sb]

    @pl.when(step == pl.num_programs(0) - 1)
    def _():
        acc = acc_ref[...]
        hi, lo = split2(acc)
        db_ref[...] = dot(hi, c_ref[...]) + dot(lo, c_ref[...])
        hi_t, lo_t = split2(acc.T)
        dc_ref[...] = dot(hi_t, b_ref[...]) + dot(lo_t, b_ref[...])


def carried_kernel(
    n, per, width, me_ref, skip_ref, rate_ref, run_ref, dt_ref, sig_ref, into_ref, grow_ref,
    b_ref, c_ref, inner_ref, db_in_ref, dc_in_ref, x_ref, g_ref, gx_ref, *refs
):
    arrived = refs[: n - 1]
    tokens_ref, steps_ref, db_ref, dc_ref, param_ref = refs[n - 1 : n + 4]
    direct_ref, carry_ref, small_ref, pad_ref = refs[n + 4 :]
    step = pl.program_id(0)
    length = run_ref.shape[0]
    states = b_ref.shape[1]
    heads = steps_ref.shape[1]
    span = x_ref.shape[1]
    nt = ((1,), (1,))
    me = me_ref[0]
    first = step * per

    @pl.when(step == 0)
    def _():
        db_ref[...] = db_in_ref[...]
        dc_ref[...] = dc_in_ref[...]
        direct_ref[...] = jnp.zeros_like(direct_ref)
        carry_ref[...] = jnp.zeros_like(carry_ref)
        small_ref[...] = jnp.zeros_like(small_ref)
        pad_ref[...] = jnp.zeros_like(pad_ref)

    def gather(order, limit):
        total = jnp.zeros((states, span), F32)
        passed = jnp.zeros((1, span), F32)
        for j, slot in enumerate(order):
            take = jnp.where(j + 1 <= limit, 1.0, 0.0)
            block = arrived[slot]
            total = total + (take * jnp.exp(passed)) * block[:states, :].astype(F32)
            low = block[states : states + EXTRA, :].astype(F32)[EXTRA - 1 : EXTRA]
            passed = passed + jnp.where(j + 1 <= limit, low, 0.0)
        return total

    entering = gather([k - 1 for k in range(1, n)], me)
    leaving = gather([n - j - 1 for j in range(1, n)], n - 1 - me)
    s_hi, s_lo = split2(entering)
    g_hi, g_lo = split2(leaving)
    grow = expand(turn(grow_ref[...], first), 0, per, width)
    into = expand(turn(into_ref[...], first), 0, per, width)
    x = x_ref[...].astype(F32)
    g = g_ref[...].astype(F32)
    gxc = into * (dot(b_ref[...], g_hi) + dot(b_ref[...], g_lo))
    yc = dot(c_ref[...], s_hi) + dot(c_ref[...], s_lo)
    gx = gx_ref[...] + gxc
    lane_head = lax.broadcasted_iota(jnp.int32, (1, span), 1) // width
    gain = jnp.zeros((1, span), F32)
    for j in range(per):
        gain = jnp.where(lane_head == j, skip_ref[first + j], gain)
    tokens_ref[...] = (gx + gain * g).astype(BF16)
    gw = grow * g
    a_hi, a_lo = split2(gw)
    dc_ref[...] += dot(a_hi, s_hi, nt) + (dot(a_lo, s_hi, nt) + dot(a_hi, s_lo, nt))
    b_hi, b_lo = split2(into * x)
    db_ref[...] += dot(b_hi, g_hi, nt) + (dot(b_lo, g_hi, nt) + dot(b_hi, g_lo, nt))
    pick = (
        first + lax.broadcasted_iota(jnp.int32, (span, LANES), 0) // width
        == lax.broadcasted_iota(jnp.int32, (span, LANES), 1)
    )
    pick = jnp.where(pick, 1.0, 0.0).astype(BF16)
    d_hi, d_lo = split2(x * gx)
    direct_ref[...] += dot(d_hi, pick) + dot(d_lo, pick)
    e_hi, e_lo = split2(gw * yc)
    carry_ref[...] += dot(e_hi, pick) + dot(e_lo, pick)
    keep = grow[length - 1 : length]
    at_end = jnp.sum(x * gxc, axis=0, keepdims=True) + keep * jnp.sum(
        entering * leaving, axis=0, keepdims=True
    )
    both = jnp.sum(x * g, axis=0, keepdims=True)
    row = lax.broadcasted_iota(jnp.int32, (EXTRA, span), 0)
    packed = jnp.where(row == 0, at_end, jnp.where(row == 1, both, 0.0))
    p1, p2, p3 = split3(packed)
    small_ref[...] += dot(p1, pick) + (dot(p2, pick) + dot(p3, pick))

    @pl.when(step == pl.num_programs(0) - 1)
    def _():
        pad_ref[:heads, :] = inner_ref[...]
        direct = direct_ref[...]
        grad_run = pad_ref[...].T + carry_ref[...] - direct
        small = small_ref[...]
        at = lax.broadcasted_iota(jnp.int32, (length, LANES), 0)
        grad_run = grad_run + jnp.where(at == length - 1, small[0:1], 0.0)
        r = lax.broadcasted_iota(jnp.int32, (length, length), 0)
        c = lax.broadcasted_iota(jnp.int32, (length, length), 1)
        upper = jnp.where(r <= c, 1.0, 0.0).astype(BF16)
        grad_decay = exact_sum(upper, grad_run)
        dt = dt_ref[...]
        pad_ref[0:1, :LANES] = jnp.ones((1, LANES), F32)
        pad_ref[0:1, :heads] = jnp.exp(rate_ref[...])
        rate = pad_ref[0:1, :LANES]
        grad_raw = (direct / dt - rate * grad_decay) * sig_ref[...]
        steps_ref[...] = grad_raw[:, :heads]
        rates = jnp.sum(-rate * dt * grad_decay, axis=0, keepdims=True)
        bias = jnp.sum(grad_raw, axis=0, keepdims=True)
        line = lax.broadcasted_iota(jnp.int32, (EXTRA, LANES), 0)
        param_ref[...] = jnp.where(
            line == 0, rates, jnp.where(line == 1, small[1:2], jnp.where(line == 2, bias, 0.0))
        )


def whole(shape):
    return pl.BlockSpec(shape, lambda i: tuple(0 for _ in shape))


def on_device(
    tokens_in, step_raw, input_map, output_map, decay_log, skip_gain, step_bias, grad_out
):
    x, raw, b, c, g = tokens_in[0], step_raw[0], input_map[0], output_map[0], grad_out[0]
    length, channels = x.shape
    heads = decay_log.shape[0]
    width = channels // heads
    states = b.shape[1]
    n = lax.axis_size("seq")
    groups = lax.axis_size("dp")
    factor = 1.0 / math.sqrt(groups * n * length * width)
    per = math.gcd(8, heads)
    span = per * width
    grid = (heads // per,)
    me = lax.axis_index("seq").astype(jnp.int32)[None]
    smem = pl.BlockSpec(memory_space=pltpu.SMEM)
    scalars = jax.ShapeDtypeStruct((length, LANES), F32)
    cols = pl.BlockSpec((length, span), lambda i: (0, i))
    tall = states + EXTRA
    message = pl.BlockSpec((tall, span), lambda i: (0, i))
    rows = [whole((length, LANES))]
    rate_row, bias_row = decay_log[None], step_bias[None]

    def cost(flops, transfer):
        return pl.CostEstimate(flops=flops, bytes_accessed=transfer, transcendentals=0)

    params = pltpu.CompilerParams(dimension_semantics=("arbitrary",))
    made = pl.pallas_call(
        functools.partial(state_kernel, n, per, width),
        grid=grid,
        in_specs=[smem, whole((length, heads)), whole((1, heads)), whole((1, heads)),
                  whole((length, states)), whole((length, states)), cols, cols],
        out_specs=[message] * (n - 1) + rows * 2 + [whole((LANES, length))] + rows * 3,
        out_shape=[jax.ShapeDtypeStruct((tall, channels), WIRE)] * (n - 1)
        + [scalars, scalars, jax.ShapeDtypeStruct((LANES, length), F32)] + [scalars] * 3,
        scratch_shapes=[pltpu.VMEM((length, LANES), F32), pltpu.VMEM((states, length), BF16),
                        pltpu.VMEM((states, length), BF16)],
        compiler_params=params,
        name="states",
    )(me, raw, bias_row, rate_row, b, c, x, g)
    sends = made[: n - 1]
    dt, run, run_t, sig, into, grow = made[n - 1 :]
    arrived = [
        lax.ppermute(sends[k - 1], "seq", [(d, (d + k) % n) for d in range(n)])
        for k in range(1, n)
    ]
    gx, inner, db_in, dc_in = pl.pallas_call(
        functools.partial(inside_kernel, per, width),
        grid=grid,
        in_specs=[whole((length, LANES)), pl.BlockSpec((per, length), lambda i: (i, 0)),
                  whole((length, LANES)),
                  whole((length, states)), whole((length, states)), cols, cols],
        out_specs=[cols, pl.BlockSpec((per, length), lambda i: (i, 0)),
                   whole((length, states)), whole((length, states))],
        out_shape=[jax.ShapeDtypeStruct((length, channels), F32),
                   jax.ShapeDtypeStruct((heads, length), F32),
                   jax.ShapeDtypeStruct((length, states), F32),
                   jax.ShapeDtypeStruct((length, states), F32)],
        scratch_shapes=[pltpu.VMEM((length, length), F32), pltpu.VMEM((length, length), F32)],
        compiler_params=params,
        cost_estimate=cost(10**10, 10**7),
        name="inside",
    )(run, run_t, dt, b, c, x, g)
    grad_tokens, grad_steps, db, dc, param = pl.pallas_call(
        functools.partial(carried_kernel, n, per, width),
        grid=grid,
        in_specs=[smem, smem, whole((1, heads))] + rows * 5
        + [whole((length, states)), whole((length, states)), whole((heads, length)),
           whole((length, states)), whole((length, states)), cols, cols, cols]
        + [message] * (n - 1),
        out_specs=[cols, whole((length, heads)), whole((length, states)),
                   whole((length, states)), whole((EXTRA, LANES))],
        out_shape=[jax.ShapeDtypeStruct((length, channels), BF16),
                   jax.ShapeDtypeStruct((length, heads), F32),
                   jax.ShapeDtypeStruct((length, states), F32),
                   jax.ShapeDtypeStruct((length, states), F32),
                   jax.ShapeDtypeStruct((EXTRA, LANES), F32)],
        scratch_shapes=[pltpu.VMEM((length, LANES), F32), pltpu.VMEM((length, LANES), F32),
                        pltpu.VMEM((EXTRA, LANES), F32), pltpu.VMEM((LANES, length), F32)],
        compiler_params=params,
        name="carried",
    )(me, skip_gain, rate_row, run, dt, sig, into, grow, b, c, inner, db_in, dc_in, x, g, gx,
      *arrived)
    total = lax.psum(param, ("seq", "dp")) * factor
    return (
        grad_tokens[None],
        grad_steps[None],
        db[None],
        dc[None],
        total[0, :heads],
        total[1, :heads],
        total[2, :heads],
    )


def solution(mesh):
    wide = P("dp", "seq", None)
    return jax.shard_map(
        on_device,
        mesh=mesh,
        in_specs=(wide, wide, wide, wide, P(), P(), P(), wide),
        out_specs=(wide, wide, wide, wide, P(), P(), P()),
        check_vma=False,
    )
```

```python
import functools
import math

import jax
import jax.numpy as jnp
from jax import lax
from jax.experimental import pallas as pl
from jax.experimental.pallas import tpu as pltpu
from jax.sharding import PartitionSpec as P

F32 = jnp.float32
BF16 = jnp.bfloat16
LANES = 128
EXTRA = 8
WIRE = jnp.float16
FLOOR = -1000.0


def dot(a, b, dims=((1,), (0,))):
    return lax.dot_general(a, b, (dims, ((), ())), preferred_element_type=F32)


def split2(v):
    hi = v.astype(BF16)
    return hi, (v - hi.astype(F32)).astype(BF16)


def split3(v):
    hi = v.astype(BF16)
    rest = v - hi.astype(F32)
    mid = rest.astype(BF16)
    return hi, mid, (rest - mid.astype(F32)).astype(BF16)


def exact_sum(mask, v):
    a, b, c = split3(v)
    return dot(mask, a) + (dot(mask, b) + dot(mask, c))


def expand(columns, first, count, width):
    rows = columns.shape[0]
    per = LANES // width
    lane = lax.broadcasted_iota(jnp.int32, (rows, LANES), 1)
    out = []
    for j in range(0, count, per):
        value = jnp.broadcast_to(columns[:, first + j : first + j + 1], (rows, LANES))
        for k in range(1, per):
            more = jnp.broadcast_to(columns[:, first + j + k : first + j + k + 1], (rows, LANES))
            value = jnp.where(lane < k * width, value, more)
        out.append(value)
    return jnp.concatenate(out, axis=1)


def turn(columns, by):
    return pltpu.roll(columns, lax.rem(LANES - by, LANES), 1)


def state_kernel(
    n, per, width, me_ref, raw_ref, bias_ref, rate_ref, b_ref, c_ref, x_ref, g_ref, *refs
):
    sends = refs[: n - 1]
    dt_ref, run_ref, run_t_ref, sig_ref, into_ref, grow_ref, scr, bt_ref, ct_ref = refs[n - 1 :]
    step = pl.program_id(0)
    heads = raw_ref.shape[1]
    length = raw_ref.shape[0]

    @pl.when(step == 0)
    def _():
        scr[...] = jnp.zeros_like(scr)
        scr[:, :heads] = raw_ref[...].astype(F32) + bias_ref[...]
        value = scr[...]
        dt = jnp.maximum(value, 0.0) + jnp.log1p(jnp.exp(-jnp.abs(value)))
        dt_ref[...] = dt
        sig_ref[...] = 1.0 / (1.0 + jnp.exp(-value))
        scr[0:1, :heads] = jnp.exp(rate_ref[...])
        decay = -scr[0:1, :] * dt
        row = lax.broadcasted_iota(jnp.int32, (length, length), 0)
        col = lax.broadcasted_iota(jnp.int32, (length, length), 1)
        lower = jnp.where(row >= col, 1.0, 0.0).astype(BF16)
        running = exact_sum(lower, decay)
        run_ref[...] = running
        run_t_ref[...] = running.T
        into_ref[...] = jnp.exp(running[length - 1 : length] - running) * dt
        grow_ref[...] = jnp.exp(running)
        bt_ref[...] = b_ref[...].astype(F32).T.astype(BF16)
        ct_ref[...] = c_ref[...].astype(F32).T.astype(BF16)

    me = me_ref[0]
    first = step * per
    into = turn(into_ref[...], first)
    grow = turn(grow_ref[...], first)
    last = turn(run_ref[length - EXTRA : length, :], first)
    xw = x_ref[...].astype(F32) * expand(into, 0, per, width)
    gw = g_ref[...].astype(F32) * expand(grow, 0, per, width)
    x_hi, x_lo = split2(xw)
    g_hi, g_lo = split2(gw)
    states = bt_ref.shape[0]
    state = dot(bt_ref[...], x_hi) + dot(bt_ref[...], x_lo)
    grad = dot(ct_ref[...], g_hi) + dot(ct_ref[...], g_lo)
    ends = jnp.maximum(expand(last, 0, per, width)[EXTRA - 1 : EXTRA], FLOOR)
    p1, p2, p3 = (part.astype(F32) for part in split3(ends))
    line = lax.broadcasted_iota(jnp.int32, (EXTRA, ends.shape[1]), 0)
    extra = jnp.where(line == 0, p1, jnp.where(line == 1, p2, jnp.where(line == 2, p3, 0.0)))
    for k in range(1, n):
        sends[k - 1][:states, :] = jnp.where(me + k < n, state, grad)
        sends[k - 1][states:, :] = extra


def inside_kernel(
    per, width, run_ref, run_t_ref, dt_ref, b_ref, c_ref, x_ref, g_ref,
    gx_ref, rows_ref, db_ref, dc_ref, cb_ref, acc_ref,
):
    step = pl.program_id(0)
    length = run_ref.shape[0]
    tile = LANES
    nt = ((1,), (1,))

    @pl.when(step == 0)
    def _():
        cb_ref[...] = dot(b_ref[...], c_ref[...], nt)
        acc_ref[...] = jnp.zeros_like(acc_ref)

    run = turn(run_ref[...], step * per)
    dt = turn(dt_ref[...], step * per)
    group = LANES // width
    lane = lax.broadcasted_iota(jnp.int32, (1, LANES), 1)
    causal = lax.broadcasted_iota(jnp.int32, (tile, tile), 0) <= lax.broadcasted_iota(
        jnp.int32, (tile, tile), 1
    )
    for pair in range(per // group):
        x_pair = x_ref[:, pair * LANES : (pair + 1) * LANES]
        g_pair = g_ref[:, pair * LANES : (pair + 1) * LANES]
        zero = jnp.zeros_like(g_pair)
        totals = [None] * (length // tile)
        for k in range(group):
            head = pair * group + k
            own = (lane >= k * width) & (lane < (k + 1) * width)
            g_own = jnp.where(own, g_pair, zero)
            column_sums = [None] * (length // tile)
            for sb in range(length // tile):
                rows = slice(sb * tile, (sb + 1) * tile)
                t0 = sb * tile
                dw = dot(x_pair[rows], g_own[t0:], nt)
                run_s = jnp.broadcast_to(run[rows, head : head + 1], (tile, tile))
                dt_s = jnp.broadcast_to(dt[rows, head : head + 1], (tile, tile))
                parts_hi, parts_lo = [], []
                for tb in range(sb, length // tile):
                    cols = slice(tb * tile, (tb + 1) * tile)
                    spread = run_t_ref[head : head + 1, cols] - run_s
                    if tb == sb:
                        spread = jnp.where(causal, spread, -jnp.inf)
                    q = jnp.exp(spread) * dt_s
                    dw_t = dw[:, tb * tile - t0 : (tb + 1) * tile - t0]
                    w = q * cb_ref[rows, cols]
                    acc_ref[rows, cols] += q * dw_t
                    part = jnp.sum(w * dw_t, axis=0, keepdims=True)
                    column_sums[tb] = part if column_sums[tb] is None else column_sums[tb] + part
                    hi, lo = split2(w)
                    parts_hi.append(hi)
                    parts_lo.append(lo)
                w_hi = jnp.concatenate(parts_hi, axis=1)
                w_lo = jnp.concatenate(parts_lo, axis=1)
                out = dot(w_hi, g_own[t0:]) + dot(w_lo, g_own[t0:])
                totals[sb] = out if totals[sb] is None else totals[sb] + out
            for tb in range(length // tile):
                rows_ref[head : head + 1, tb * tile : (tb + 1) * tile] = column_sums[tb]
        for sb in range(length // tile):
            gx_ref[sb * tile : (sb + 1) * tile, pair * LANES : (pair + 1) * LANES] = totals[sb]

    @pl.when(step == pl.num_programs(0) - 1)
    def _():
        acc = acc_ref[...]
        hi, lo = split2(acc)
        db_ref[...] = dot(hi, c_ref[...]) + dot(lo, c_ref[...])
        hi_t, lo_t = split2(acc.T)
        dc_ref[...] = dot(hi_t, b_ref[...]) + dot(lo_t, b_ref[...])


def carried_kernel(
    n, per, width, me_ref, skip_ref, rate_ref, run_ref, dt_ref, sig_ref, into_ref, grow_ref,
    b_ref, c_ref, inner_ref, db_in_ref, dc_in_ref, x_ref, g_ref, gx_ref, *refs
):
    arrived = refs[: n - 1]
    tokens_ref, steps_ref, db_ref, dc_ref, param_ref = refs[n - 1 : n + 4]
    direct_ref, carry_ref, small_ref, pad_ref = refs[n + 4 :]
    step = pl.program_id(0)
    length = run_ref.shape[0]
    states = b_ref.shape[1]
    heads = steps_ref.shape[1]
    span = x_ref.shape[1]
    nt = ((1,), (1,))
    me = me_ref[0]
    first = step * per

    @pl.when(step == 0)
    def _():
        db_ref[...] = db_in_ref[...]
        dc_ref[...] = dc_in_ref[...]
        direct_ref[...] = jnp.zeros_like(direct_ref)
        carry_ref[...] = jnp.zeros_like(carry_ref)
        small_ref[...] = jnp.zeros_like(small_ref)
        pad_ref[...] = jnp.zeros_like(pad_ref)

    def gather(order, limit):
        total = jnp.zeros((states, span), F32)
        passed = jnp.zeros((1, span), F32)
        for j, slot in enumerate(order):
            take = jnp.where(j + 1 <= limit, 1.0, 0.0)
            block = arrived[slot]
            total = total + (take * jnp.exp(passed)) * block[:states, :]
            low = jnp.sum(block[states : states + EXTRA, :], axis=0, keepdims=True)
            passed = passed + jnp.where(j + 1 <= limit, low, 0.0)
        return total

    entering = gather([k - 1 for k in range(1, n)], me)
    leaving = gather([n - j - 1 for j in range(1, n)], n - 1 - me)
    s_hi, s_lo = split2(entering)
    g_hi, g_lo = split2(leaving)
    grow = expand(turn(grow_ref[...], first), 0, per, width)
    into = expand(turn(into_ref[...], first), 0, per, width)
    x = x_ref[...].astype(F32)
    g = g_ref[...].astype(F32)
    gxc = into * (dot(b_ref[...], g_hi) + dot(b_ref[...], g_lo))
    yc = dot(c_ref[...], s_hi) + dot(c_ref[...], s_lo)
    gx = gx_ref[...] + gxc
    lane_head = lax.broadcasted_iota(jnp.int32, (1, span), 1) // width
    gain = jnp.zeros((1, span), F32)
    for j in range(per):
        gain = jnp.where(lane_head == j, skip_ref[first + j], gain)
    tokens_ref[...] = (gx + gain * g).astype(BF16)
    gw = grow * g
    a_hi, a_lo = split2(gw)
    dc_ref[...] += dot(a_hi, s_hi, nt) + (dot(a_lo, s_hi, nt) + dot(a_hi, s_lo, nt))
    b_hi, b_lo = split2(into * x)
    db_ref[...] += dot(b_hi, g_hi, nt) + (dot(b_lo, g_hi, nt) + dot(b_hi, g_lo, nt))
    pick = (
        first + lax.broadcasted_iota(jnp.int32, (span, LANES), 0) // width
        == lax.broadcasted_iota(jnp.int32, (span, LANES), 1)
    )
    pick = jnp.where(pick, 1.0, 0.0).astype(BF16)
    d_hi, d_lo = split2(x * gx)
    direct_ref[...] += dot(d_hi, pick) + dot(d_lo, pick)
    e_hi, e_lo = split2(gw * yc)
    carry_ref[...] += dot(e_hi, pick) + dot(e_lo, pick)
    keep = grow[length - 1 : length]
    at_end = jnp.sum(x * gxc, axis=0, keepdims=True) + keep * jnp.sum(
        entering * leaving, axis=0, keepdims=True
    )
    both = jnp.sum(x * g, axis=0, keepdims=True)
    row = lax.broadcasted_iota(jnp.int32, (EXTRA, span), 0)
    packed = jnp.where(row == 0, at_end, jnp.where(row == 1, both, 0.0))
    p1, p2, p3 = split3(packed)
    small_ref[...] += dot(p1, pick) + (dot(p2, pick) + dot(p3, pick))

    @pl.when(step == pl.num_programs(0) - 1)
    def _():
        pad_ref[:heads, :] = inner_ref[...]
        direct = direct_ref[...]
        grad_run = pad_ref[...].T + carry_ref[...] - direct
        small = small_ref[...]
        at = lax.broadcasted_iota(jnp.int32, (length, LANES), 0)
        grad_run = grad_run + jnp.where(at == length - 1, small[0:1], 0.0)
        r = lax.broadcasted_iota(jnp.int32, (length, length), 0)
        c = lax.broadcasted_iota(jnp.int32, (length, length), 1)
        upper = jnp.where(r <= c, 1.0, 0.0).astype(BF16)
        grad_decay = exact_sum(upper, grad_run)
        dt = dt_ref[...]
        pad_ref[0:1, :LANES] = jnp.ones((1, LANES), F32)
        pad_ref[0:1, :heads] = jnp.exp(rate_ref[...])
        rate = pad_ref[0:1, :LANES]
        grad_raw = (direct / dt - rate * grad_decay) * sig_ref[...]
        steps_ref[...] = grad_raw[:, :heads]
        rates = jnp.sum(-rate * dt * grad_decay, axis=0, keepdims=True)
        bias = jnp.sum(grad_raw, axis=0, keepdims=True)
        line = lax.broadcasted_iota(jnp.int32, (EXTRA, LANES), 0)
        param_ref[...] = jnp.where(
            line == 0, rates, jnp.where(line == 1, small[1:2], jnp.where(line == 2, bias, 0.0))
        )


def sum_kernel(groups, n, factor, in_ref, out_ref, dp_slots, seq_slots, part, send_dp, recv_dp,
               send_seq, recv_seq):
    stages = (
        ("dp", groups, in_ref, dp_slots, send_dp, recv_dp, part, 1.0),
        ("seq", n, part, seq_slots, send_seq, recv_seq, out_ref, factor),
    )
    barrier = pltpu.get_barrier_semaphore()
    for axis, size, *_ in stages:
        me = lax.axis_index(axis)
        for k in range(1, size):
            pl.semaphore_signal(
                barrier, inc=1, device_id={axis: lax.rem(me + k, size)},
                device_id_type=pl.DeviceIdType.MESH,
            )
    pl.semaphore_wait(barrier, groups + n - 2)
    for axis, size, src, slots, send, recv, dst, scale in stages:
        me = lax.axis_index(axis)
        copies = []
        for k in range(1, size):
            copy = pltpu.make_async_remote_copy(
                src_ref=src, dst_ref=slots.at[me], send_sem=send.at[k], recv_sem=recv.at[k],
                device_id={axis: lax.rem(me + k, size)}, device_id_type=pl.DeviceIdType.MESH,
            )
            copy.start()
            copies.append(copy)
        slots[me] = src[...]
        for copy in copies:
            copy.wait()
        total = slots[0]
        for j in range(1, size):
            total = total + slots[j]
        dst[...] = total * scale


def sum_all(param, groups, n, factor):
    vmem = pl.BlockSpec(memory_space=pltpu.VMEM)
    return pl.pallas_call(
        functools.partial(sum_kernel, groups, n, factor),
        out_shape=jax.ShapeDtypeStruct(param.shape, F32),
        in_specs=[vmem],
        out_specs=vmem,
        scratch_shapes=[
            pltpu.VMEM((groups,) + param.shape, F32),
            pltpu.VMEM((n,) + param.shape, F32),
            pltpu.VMEM(param.shape, F32),
            pltpu.SemaphoreType.DMA((groups,)),
            pltpu.SemaphoreType.DMA((groups,)),
            pltpu.SemaphoreType.DMA((n,)),
            pltpu.SemaphoreType.DMA((n,)),
        ],
        compiler_params=pltpu.CompilerParams(collective_id=0, has_side_effects=True),
        name="sums",
    )(param)


def whole(shape):
    return pl.BlockSpec(shape, lambda i: tuple(0 for _ in shape))


def on_device(
    tokens_in, step_raw, input_map, output_map, decay_log, skip_gain, step_bias, grad_out
):
    x, raw, b, c, g = tokens_in[0], step_raw[0], input_map[0], output_map[0], grad_out[0]
    length, channels = x.shape
    heads = decay_log.shape[0]
    width = channels // heads
    states = b.shape[1]
    n = lax.axis_size("seq")
    groups = lax.axis_size("dp")
    factor = 1.0 / math.sqrt(groups * n * length * width)
    per = math.gcd(8, heads)
    span = per * width
    grid = (heads // per,)
    me = lax.axis_index("seq").astype(jnp.int32)[None]
    smem = pl.BlockSpec(memory_space=pltpu.SMEM)
    scalars = jax.ShapeDtypeStruct((length, LANES), F32)
    cols = pl.BlockSpec((length, span), lambda i: (0, i))
    tall = states + EXTRA
    message = pl.BlockSpec((tall, span), lambda i: (0, i))
    rows = [whole((length, LANES))]
    rate_row, bias_row = decay_log[None], step_bias[None]

    def cost(flops, transfer):
        return pl.CostEstimate(flops=flops, bytes_accessed=transfer, transcendentals=0)

    params = pltpu.CompilerParams(dimension_semantics=("arbitrary",))
    made = pl.pallas_call(
        functools.partial(state_kernel, n, per, width),
        grid=grid,
        in_specs=[smem, whole((length, heads)), whole((1, heads)), whole((1, heads)),
                  whole((length, states)), whole((length, states)), cols, cols],
        out_specs=[message] * (n - 1) + rows * 2 + [whole((LANES, length))] + rows * 3,
        out_shape=[jax.ShapeDtypeStruct((tall, channels), F32)] * (n - 1)
        + [scalars, scalars, jax.ShapeDtypeStruct((LANES, length), F32)] + [scalars] * 3,
        scratch_shapes=[pltpu.VMEM((length, LANES), F32), pltpu.VMEM((states, length), BF16),
                        pltpu.VMEM((states, length), BF16)],
        compiler_params=params,
        name="states",
    )(me, raw, bias_row, rate_row, b, c, x, g)
    sends = made[: n - 1]
    dt, run, run_t, sig, into, grow = made[n - 1 :]
    arrived = [
        lax.ppermute(sends[k - 1].astype(WIRE), "seq", [(d, (d + k) % n) for d in range(n)])
        for k in range(1, n)
    ]
    gx, inner, db_in, dc_in = pl.pallas_call(
        functools.partial(inside_kernel, per, width),
        grid=grid,
        in_specs=[whole((length, LANES)), pl.BlockSpec((per, length), lambda i: (i, 0)),
                  whole((length, LANES)),
                  whole((length, states)), whole((length, states)), cols, cols],
        out_specs=[cols, pl.BlockSpec((per, length), lambda i: (i, 0)),
                   whole((length, states)), whole((length, states))],
        out_shape=[jax.ShapeDtypeStruct((length, channels), F32),
                   jax.ShapeDtypeStruct((heads, length), F32),
                   jax.ShapeDtypeStruct((length, states), F32),
                   jax.ShapeDtypeStruct((length, states), F32)],
        scratch_shapes=[pltpu.VMEM((length, length), F32), pltpu.VMEM((length, length), F32)],
        compiler_params=params,
        cost_estimate=cost(10**10, 10**7),
        name="inside",
    )(run, run_t, dt, b, c, x, g)
    grad_tokens, grad_steps, db, dc, param = pl.pallas_call(
        functools.partial(carried_kernel, n, per, width),
        grid=grid,
        in_specs=[smem, smem, whole((1, heads))] + rows * 5
        + [whole((length, states)), whole((length, states)), whole((heads, length)),
           whole((length, states)), whole((length, states)), cols, cols, cols]
        + [message] * (n - 1),
        out_specs=[cols, whole((length, heads)), whole((length, states)),
                   whole((length, states)), whole((EXTRA, LANES))],
        out_shape=[jax.ShapeDtypeStruct((length, channels), BF16),
                   jax.ShapeDtypeStruct((length, heads), F32),
                   jax.ShapeDtypeStruct((length, states), F32),
                   jax.ShapeDtypeStruct((length, states), F32),
                   jax.ShapeDtypeStruct((EXTRA, LANES), F32)],
        scratch_shapes=[pltpu.VMEM((length, LANES), F32), pltpu.VMEM((length, LANES), F32),
                        pltpu.VMEM((EXTRA, LANES), F32), pltpu.VMEM((LANES, length), F32)],
        compiler_params=params,
        name="carried",
    )(me, skip_gain, rate_row, run, dt, sig, into, grow, b, c, inner, db_in, dc_in, x, g, gx,
      *[part.astype(F32) for part in arrived])
    total = sum_all(param, groups, n, factor)
    return (
        grad_tokens[None],
        grad_steps[None],
        db[None],
        dc[None],
        total[0, :heads],
        total[1, :heads],
        total[2, :heads],
    )


def solution(mesh):
    wide = P("dp", "seq", None)
    return jax.shard_map(
        on_device,
        mesh=mesh,
        in_specs=(wide, wide, wide, wide, P(), P(), P(), wide),
        out_specs=(wide, wide, wide, wide, P(), P(), P()),
        check_vma=False,
    )
```
